32 devices in a mesh: cls: 4 (over y, x), str: 8 (over z, core).
Axes of the slice: x: 2, y: 2, z: 4, core: 2. Of those that a mesh axis runs over, the one named last changes fastest.
Arguments:
- first_factor_tiles: float32 [8, 1024, 2, 4, 1024], P(None, ('cls', 'str')), may hold values from -6 to 6
- b_blocks: float32 [8, 1024, 2, 4, 512], P(None, ('cls', 'str')), may hold values from -0.0625 to 0.0625
Outputs:
- c_blocks: float32 [8, 1024, 2, 4, 512], P(None, ('cls', 'str'))
The draws below stay inside these ranges and needn't reach their ends.
All inputs are finite; a program needn't handle non-finite values.
Results may differ from the reference program's by a relative error of at most 0.0003.
Values sent between devices are 32-bit elements; how exact they have to be, the bound alone decides.
A program may use at most 128 MiB of HBM per device.

```python
import jax
import jax.numpy as jnp
import numpy as np
from jax import lax

N = 8192
Q = 1024
QC = 512


def block_levels(key, extent, split, low, largest):
    level = 1.0
    for position, parts in split:
        draws = jax.random.uniform(jax.random.fold_in(jax.random.fold_in(key, 6), position), (parts,), jnp.float32, low / len(split), largest / len(split))
        level = level * jnp.repeat(jnp.exp(draws), extent[position] // parts).reshape((-1,) + (1,) * (len(extent) - 1 - position))
    return level


def scatter_about(key, dims, width, bound, shards=(), kind=jnp.bfloat16):
    drawn = width * jax.random.normal(key, dims, jnp.float32)
    if shards:
        drawn = drawn * block_levels(key, dims, shards, -0.22, 0.18)
    return jnp.clip(drawn, -bound, bound).astype(kind)


def setup_inputs(seed: int = 0) -> dict:
    key_of = jax.random.split(jax.random.key(seed), 3)
    return {
        "first_factor_tiles": scatter_about(key_of[0], (8, Q, 2, 4, Q), 1.0, 6.0, ((1, 32),), jnp.float32),
        "b_blocks": scatter_about(key_of[1], (8, Q, 2, 4, QC), N ** -0.5, 0.0625, ((1, 32),), jnp.float32),
    }


def strassen_weight_lists():
    left_base = np.array([[1, 0, 0, 0], [0, 1, 0, 0], [1, 1, -1, -1], [0, 0, 0, 1], [0, 0, 1, 1], [-1, 0, 1, 1], [1, 0, -1, 0]], np.float32)
    right_base_matrix = np.array([[1, 0, 0, 0], [0, 0, 1, 0], [0, 0, 0, 1], [1, -1, -1, 1], [-1, 1, 0, 0], [1, -1, 0, 1], [0, -1, 0, 1]], np.float32)
    product_grid_start = np.array([[1, 1, 0, 0, 0, 0, 0], [1, 0, 1, 0, 1, 1, 0], [1, 0, 0, -1, 0, 1, 1], [1, 0, 0, 0, 1, 1, 1]], np.float32)
    left_split = left_base.reshape(7, 2, 2)
    right_split = right_base_matrix.reshape(7, 2, 2)
    outer_split = product_grid_start.reshape(2, 2, 7)
    left_table = (left_split[:, None, :, None, :, None] * left_split[None, :, None, :, None, :]).reshape(49, 4, 4)
    right_table = (right_split[:, None, :, None, :, None] * right_split[None, :, None, :, None, :]).reshape(49, 4, 4)
    outer_table = (outer_split[:, None, :, None, :, None] * outer_split[None, :, None, :, None, :]).reshape(4, 4, 49)
    return left_table, right_table, outer_table


def reference(first_factor_tiles, b_blocks):
    first_factor_host_grid, second_factor_host_grid, product_host_grid = strassen_weight_lists()
    left_table = jnp.asarray(first_factor_host_grid).astype(first_factor_tiles.dtype)
    right_table = jnp.asarray(second_factor_host_grid).astype(first_factor_tiles.dtype)
    outer_table = jnp.asarray(product_host_grid).astype(first_factor_tiles.dtype)
    product_ids = np.arange(8)
    inner_halves = product_ids // 4
    row_half_split = (product_ids // 2) % 2
    col_halves = product_ids % 2
    a_six = first_factor_tiles.reshape(2, 4, Q, 2, 4, Q)
    b_six = b_blocks.reshape(2, 4, Q, 2, 4, QC)
    left_stack = a_six[row_half_split, :, :, inner_halves]
    right_stack = b_six[inner_halves, :, :, col_halves]
    highest = lax.Precision.HIGHEST

    def leaf_product(pair):
        x_quad, y_quad = pair
        left_leaves = jnp.einsum('mac,aqcr->mqr', left_table, x_quad, precision=highest)
        right_leaves = jnp.einsum('mac,aqcr->mqr', right_table, y_quad, precision=highest)
        leaf_out = jnp.einsum('mqk,mkr->mqr', left_leaves, right_leaves, precision=highest)
        return jnp.einsum('acm,mqr->aqcr', outer_table, leaf_out, precision=highest)

    partials = lax.map(leaf_product, (left_stack, right_stack))
    partials = partials.reshape(2, 2, 2, 4, Q, 4, QC)
    summed = partials[0] + partials[1]
    summed = jnp.transpose(summed, (0, 2, 3, 1, 4, 5))
    return summed.reshape(8, Q, 2, 4, QC)
```

```python
import functools

import jax
import jax.numpy as jnp
from jax import lax
from jax.experimental import pallas as pl
from jax.experimental.pallas import tpu as pltpu
from jax.sharding import PartitionSpec as P

MESH = pl.DeviceIdType.MESH
LAG = 3
AHEAD = 2


def flip(index, mask, count):
    out, bit = index, 1
    while bit < count:
        have, want = (index // bit) % 2, (mask // bit) % 2
        out = out + want * (1 - 2 * have) * bit
        bit *= 2
    return out


def kernel(
    classes, subs, a_ref, b_ref, o_ref, aland, ball,
    ahi, alo, astage, bstage, bhi, blo, cpart, rland,
    a_send, a_recv, own_send, fwd_send, line_recv, peer_send, peer_recv,
    c_send, c_recv, a_load, b_load, o_sem,
):
    chunks, groups, piece, width = b_ref.shape
    rows = a_ref.shape[1]
    depth = subs * piece
    spots = subs // 2
    c, s = lax.axis_index("cls"), lax.axis_index("str")
    spot, core = s // 2, s % 2
    mate = (c, s + 1 - 2 * core)
    beside = ((c, s - 2), (c, s + 2))
    has = (spot > 0, spot < spots - 1)

    barrier = pltpu.get_barrier_semaphore()
    for d in range(1, classes):
        pl.semaphore_signal(barrier, inc=1, device_id=(flip(c, d, classes), s), device_id_type=MESH)
    pl.semaphore_signal(barrier, inc=1, device_id=mate, device_id_type=MESH)
    for side in range(2):
        @pl.when(has[side])
        def _():
            pl.semaphore_signal(barrier, inc=1, device_id=beside[side], device_id_type=MESH)
    lower, higher = (spot + spots - 1) // spots, (2 * spots - 2 - spot) // spots
    pl.semaphore_wait(barrier, classes + lower + higher)

    def remote(src, dst, send, recv, to):
        return pltpu.make_async_remote_copy(
            src_ref=src, dst_ref=dst, send_sem=send, recv_sem=recv,
            device_id=to, device_id_type=MESH,
        )

    def slot(j, owner):
        return ball.at[j, :, pl.ds(pl.multiple_of(owner * piece, piece), piece), :]

    def own_line(j, side):
        return remote(b_ref.at[j], slot(j, s), own_send.at[side, j], line_recv.at[side, j, 0], beside[side])

    def own_mate(j):
        return remote(b_ref.at[j], slot(j, s), peer_send.at[j, spot], peer_recv.at[j, spot], mate)

    def origin(side, dist):
        return spot + dist if side == 0 else spot - dist

    def there(side, dist):
        return spot + dist < spots if side == 0 else spot >= dist

    def arrival(j, side, dist):
        at = slot(j, 2 * origin(side, dist) + core)
        return remote(at, at, own_send.at[side, j], line_recv.at[side, j, dist - 1], beside[1 - side])

    def onward(j, side, dist):
        at = slot(j, 2 * origin(side, dist) + core)
        return remote(at, at, fwd_send.at[side, j, dist - 1], line_recv.at[side, j, dist], beside[side])

    def across(j, side, dist):
        begin = origin(side, dist)
        at = slot(j, 2 * begin + core)
        return remote(at, at, peer_send.at[j, begin], peer_recv.at[j, begin], mate)

    def forward(j, dist):
        for side in range(2):
            @pl.when(there(side, dist))
            def _():
                arrival(j, side, dist).wait_recv()

                @pl.when(has[side])
                def _():
                    onward(j, side, dist).start()

                across(j, side, dist).start()

    def a_copy(d):
        peer = flip(c, d, classes)
        return remote(
            a_ref.at[:, :, pl.ds(pl.multiple_of(peer * depth, depth), depth)],
            aland.at[:, pl.ds(pl.multiple_of(c * rows, rows), rows), :],
            a_send.at[d], a_recv.at[d], (peer, s),
        )

    for d in range(1, classes):
        a_copy(d).start()

    def begin(j, _):
        for side in range(2):
            @pl.when(has[side])
            def _():
                own_line(j, side).start()
        own_mate(j).start()
        return 0

    lax.fori_loop(0, chunks, begin, 0)

    for j in range(min(AHEAD, chunks)):
        forward(j, 1)
    for d in range(1, classes):
        a_copy(d).wait_recv()

    def load_a(g, held):
        for e in range(classes):
            to = astage.at[held, pl.ds(e * rows, rows), :]

            @pl.when(c == e)
            def _():
                pltpu.make_async_copy(
                    a_ref.at[g, :, pl.ds(pl.multiple_of(c * depth, depth), depth)], to, a_load.at[held]
                ).start()

            @pl.when(c != e)
            def _():
                pltpu.make_async_copy(aland.at[g, pl.ds(e * rows, rows), :], to, a_load.at[held]).start()

    load_a(0, 0)
    for g in range(groups):
        held = g % 2
        if g + 1 < groups:
            load_a(g + 1, 1 - held)
        pltpu.make_async_copy(aland.at[g], astage.at[held], a_load.at[held]).wait()

        def split(m, _, held=held, g=g):
            at = pl.ds(pl.multiple_of(m * rows, rows), rows)
            value = astage[held, at, :]
            high = value.astype(jnp.bfloat16)
            ahi[at, g * depth:(g + 1) * depth] = high
            alo[at, g * depth:(g + 1) * depth] = (value - high.astype(jnp.float32)).astype(jnp.bfloat16)
            return 0

        lax.fori_loop(0, classes, split, 0)

    def c_copy(j, d):
        peer = flip(c, d, classes)
        return remote(
            cpart.at[j, pl.ds(pl.multiple_of(peer * rows, rows), rows), :],
            rland.at[j, d - 1], c_send.at[j, d], c_recv.at[j, d], (peer, s),
        )

    mine = pl.ds(pl.multiple_of(c * rows, rows), rows)

    def out_copy(j):
        return pltpu.make_async_copy(cpart.at[j, mine, :], o_ref.at[j], o_sem.at[j])

    def reduce(j):
        for d in range(1, classes):
            c_copy(j, d).wait_recv()
        total = cpart[j, mine, :]
        for d in range(1, classes):
            total = total + rland[j, d - 1]
        cpart[j, mine, :] = total
        out_copy(j).start()

    def step(j, _):
        if spots > 1:
            @pl.when(j + AHEAD < chunks)
            def _():
                forward(j + AHEAD, 1)
        for dist in range(2, spots):
            forward(j, dist)

        for owner in range(subs):
            to = bstage.at[:, pl.ds(owner * piece, piece), :]

            @pl.when(s == owner)
            def _():
                pltpu.make_async_copy(b_ref.at[j], to, b_load.at[0]).start()

            @pl.when(s != owner)
            def _():
                @pl.when(core != owner % 2)
                def _():
                    remote(to_slot(j, owner), to_slot(j, owner), peer_send.at[j, owner // 2],
                           peer_recv.at[j, owner // 2], mate).wait_recv()

                pltpu.make_async_copy(to_slot(j, owner), to, b_load.at[0]).start()

        pltpu.make_async_copy(ball.at[j], bstage, b_load.at[0]).wait()

        def split(g, _):
            value = bstage[g]
            high = value.astype(jnp.bfloat16)
            at = pl.ds(pl.multiple_of(g * depth, depth), depth)
            bhi[at, :] = high
            blo[at, :] = (value - high.astype(jnp.float32)).astype(jnp.bfloat16)
            return 0

        lax.fori_loop(0, groups, split, 0)

        def part(i, _):
            d = (i + 1) % classes
            at = pl.ds(pl.multiple_of(flip(c, d, classes) * rows, rows), rows)
            dot = functools.partial(jnp.dot, preferred_element_type=jnp.float32)
            cpart[j, at, :] = (
                dot(ahi[at, :], bhi[...]) + dot(ahi[at, :], blo[...]) + dot(alo[at, :], bhi[...])
            )

            @pl.when(d != 0)
            def _():
                c_copy(j, d).start()

            return 0

        lax.fori_loop(0, classes, part, 0)

        @pl.when(j >= LAG)
        def _():
            reduce(j - LAG)

        return 0

    def to_slot(j, owner):
        return ball.at[j, :, pl.ds(owner * piece, piece), :]

    lax.fori_loop(0, chunks, step, 0)
    for j in range(max(chunks - LAG, 0), chunks):
        reduce(j)

    def finish(j, _):
        out_copy(j).wait()
        own_mate(j).wait_send()
        for d in range(1, classes):
            c_copy(j, d).wait_send()
        for side in range(2):
            @pl.when(has[side])
            def _():
                own_line(j, side).wait_send()
            for dist in range(1, spots):
                @pl.when(there(side, dist))
                def _():
                    @pl.when(has[side])
                    def _():
                        onward(j, side, dist).wait_send()
                    across(j, side, dist).wait_send()
        return 0

    lax.fori_loop(0, chunks, finish, 0)
    for d in range(1, classes):
        a_copy(d).wait_send()


def local(classes, subs, first_factor_tiles, b_blocks):
    blocks, q, halves, cols, order = first_factor_tiles.shape
    inner, width = halves * cols, b_blocks.shape[4]
    rows = blocks * q
    left = first_factor_tiles.reshape(rows, inner, order)
    right = jnp.transpose(b_blocks.reshape(inner, q, inner, width), (2, 0, 1, 3))
    if q % 8 == 0:
        left = jnp.transpose(left, (1, 0, 2))
    else:
        left = left.reshape(rows, inner, classes * subs, q)
        left = jnp.transpose(left, (0, 2, 1, 3)).reshape(1, rows, inner * order)
        right = right.reshape(inner, 1, inner * q, width)
    chunks, groups, piece, _ = right.shape
    depth = subs * piece
    dma = pltpu.SemaphoreType.DMA
    f32, bf16 = jnp.float32, jnp.bfloat16
    spots = subs // 2
    out, _, _ = pl.pallas_call(
        functools.partial(kernel, classes, subs),
        out_shape=(
            jax.ShapeDtypeStruct((chunks, rows, width), f32),
            jax.ShapeDtypeStruct((groups, classes * rows, depth), f32),
            jax.ShapeDtypeStruct((chunks, groups, depth, width), f32),
        ),
        in_specs=[pl.BlockSpec(memory_space=pl.ANY)] * 2,
        out_specs=(pl.BlockSpec(memory_space=pl.ANY),) * 3,
        scratch_shapes=[
            pltpu.VMEM((classes * rows, groups * depth), bf16),
            pltpu.VMEM((classes * rows, groups * depth), bf16),
            pltpu.VMEM((2, classes * rows, depth), f32),
            pltpu.VMEM((groups, depth, width), f32),
            pltpu.VMEM((groups * depth, width), bf16),
            pltpu.VMEM((groups * depth, width), bf16),
            pltpu.VMEM((chunks, classes * rows, width), f32),
            pltpu.VMEM((chunks, classes - 1, rows, width), f32),
            dma((classes,)),
            dma((classes,)),
            dma((2, chunks)),
            dma((2, chunks, spots)),
            dma((2, chunks, spots)),
            dma((chunks, spots)),
            dma((chunks, spots)),
            dma((chunks, classes)),
            dma((chunks, classes)),
            dma((2,)),
            dma((1,)),
            dma((chunks,)),
        ],
        compiler_params=pltpu.CompilerParams(
            collective_id=0, has_side_effects=True, vmem_limit_bytes=60 * 1024 * 1024
        ),
    )(left, right)
    out = jnp.transpose(out, (1, 0, 2))
    return out.reshape(b_blocks.shape)


def solution(mesh):
    spec = P(None, ("cls", "str"), None, None, None)
    return jax.shard_map(
        functools.partial(local, mesh.shape["cls"], mesh.shape["str"]),
        mesh=mesh, in_specs=(spec, spec), out_specs=spec, check_vma=False,
    )
```
